768 devices in a mesh: slot: 6 (over z_lo), tile: 8 (over z_hi, x), obs: 16 (over y, core).
Axes of the slice: x: 4, y: 8, z: 12 (z_hi: 2, z_lo: 6; z = z_hi * 6 + z_lo), core: 2. Of those that a mesh axis runs over, the one named last changes fastest.
Arguments:
- forcing: float32 [6, 128, 64, 2048], P('slot', None, 'tile', 'obs'), may hold values from -6 to 6
- winds: float32 [2, 6, 64, 2048], P(None, 'slot', 'tile', 'obs'), may hold values from -0.2 to 0.2
- mixing: float32 [128, 128], replicated, may hold values from -0.12 to 0.12
- observation_columns: int32 [4, 6, 262144], P(None, 'slot', ('tile', 'obs')), may hold values from 0 to 1023
- obs_weights: float32 [4, 6, 262144], P(None, 'slot', ('tile', 'obs')), may hold values from 0.05 to 0.5
- obs_counts: int32 [6, 128, 16], P('slot', ('tile', 'obs')), may hold values from 16 to 128, as said below
- jacobian: float32 [6, 16, 128, 128], P('slot', 'obs'), may hold values from -0.5 to 0.5
Outputs:
- states: float32 [6, 128, 64, 2048], P('slot', None, 'tile', 'obs')
- radiances: float32 [6, 128, 262144], P('slot', None, ('tile', 'obs'))
The draws below stay inside these ranges and needn't reach their ends.
Inputs may be any that keep to these rules, and one draw needn't show every extreme that they name: `obs_counts`: every block of 128 rows has its live rows first; in every slot and every tile one owner's blocks are full from every source.
All inputs are finite; a program needn't handle non-finite values.
Results may differ from the reference program's by a relative error of at most 0.0001.
Values sent between devices are 32-bit elements; how exact they have to be, the bound alone decides.
No kernel may reach another device: no remote copies, remote signals or barrier semaphores. Data moves between devices by JAX's collectives and lax.ppermute only.
A program may use at most 32 MiB of HBM per device.

```python
import jax
import jax.numpy as jnp
from jax import lax

VL = 128
CHAN = 128
STEPS = 4
CX = 8
CY = 128
CAP = 128
NX = 64
NY = 2048
ROWS_ALL = 262144
N_SLOT = 6
N_TILE = 8
N_OBS = 16


def draw_obs_counts(key, part):
    lower = jax.random.randint(jax.random.fold_in(key, 11), (N_SLOT, N_TILE, N_OBS, N_OBS), CAP // 8, CAP // 2 + 1)
    chosen = jax.random.randint(jax.random.fold_in(key, 12), (N_SLOT, N_TILE, 1, 1), 0, N_OBS)
    owners = jnp.arange(N_OBS, dtype=jnp.int32).reshape(1, 1, 1, N_OBS)
    filled = jnp.where(owners == chosen, CAP, lower)
    return filled.reshape(N_SLOT, N_TILE * N_OBS, N_OBS).astype(jnp.int32)


def set_ends(values, own_key, low, largest):
    shape = values.shape
    place = [jax.random.randint(jax.random.fold_in(own_key, axis), (), 0, shape[axis]) for axis in range(len(shape))]
    values = values.at[tuple(place)].set(low)
    longest = shape.index(max(shape))
    place[longest] = (place[longest] + 1) % shape[longest]
    return values.at[tuple(place)].set(largest)


def steps_of(rng, shape, shards, smallest, largest):
    def one(dim, blocks):
        draws = jax.random.uniform(jax.random.fold_in(jax.random.fold_in(rng, 6), dim), (blocks,), jnp.float32, smallest / len(shards), largest / len(shards))
        return jnp.repeat(jnp.exp(draws), shape[dim] // blocks).reshape((-1,) + (1,) * (len(shape) - dim - 1))

    gain = one(*shards[0])
    for cut in shards[1:]:
        gain = gain * one(*cut)
    return gain


def noise(own_key, extent, scale, bound, cuts=(), held_as=jnp.bfloat16):
    values = scale * jax.random.normal(own_key, extent, jnp.float32)
    if cuts:
        values = values * steps_of(own_key, extent, cuts, -0.22, 0.18)
    return jnp.clip(values, -bound, bound).astype(held_as)


def setup_inputs(seed: int = 0) -> dict:
    splits = jax.random.split(jax.random.key(seed), 8)
    forcing = noise(splits[0], (N_SLOT, VL, NX, NY), 1.0, 6.0, ((0, 6), (2, 8), (3, 16)), jnp.float32)
    winds = jnp.clip(jax.random.uniform(splits[1], (2, N_SLOT, NX, NY), jnp.float32, -0.2, 0.2) * steps_of(splits[1], (2, N_SLOT, NX, NY), ((1, 6), (2, 8), (3, 16)), -0.4, 0.0), -0.2, 0.2)
    mixing = noise(splits[2], (VL, VL), 0.02, 0.12, (), jnp.float32)
    observation_columns = set_ends(jax.random.randint(splits[3], (4, N_SLOT, ROWS_ALL), 0, CX * CY), jax.random.fold_in(splits[3], 1), 0, (CX * CY) - 1).astype(jnp.int32)
    obs_weights = jnp.clip(0.05 + 0.45 * jax.random.uniform(splits[4], (4, N_SLOT, ROWS_ALL), jnp.float32) ** steps_of(splits[4], (4, N_SLOT, ROWS_ALL), ((1, 6), (2, 128)), -0.2, 0.2), 0.05, 0.5)
    obs_counts = draw_obs_counts(jax.random.fold_in(splits[7], 71), 0)
    jacobian = noise(splits[6], (N_SLOT, N_OBS, CHAN, VL), VL ** -0.5, 0.5, ((0, 6), (1, 16)), jnp.float32)
    return dict(forcing=forcing, winds=winds, mixing=mixing, observation_columns=observation_columns, obs_weights=obs_weights, obs_counts=obs_counts, jacobian=jacobian)


mixing_rate = 0.15


def advance_slot(padded, eastward_rate, northward_rate, mixing):
    centre = padded[:, 1:-1, 1:-1]
    eastern = padded[:, 2:, 1:-1]
    western = padded[:, :-2, 1:-1]
    northern = padded[:, 1:-1, 2:]
    southern = padded[:, 1:-1, :-2]
    shifted_state = centre + eastward_rate * (eastern - western) + northward_rate * (northern - southern)
    shifted_state = shifted_state + mixing_rate * (eastern + western + northern + southern - 4.0 * centre)
    return shifted_state + jnp.einsum("mn,nlk->mlk", mixing, shifted_state, precision=lax.Precision.HIGHEST)


def reference(forcing, winds, mixing, observation_columns, obs_weights, obs_counts, jacobian):
    states = [forcing[0]]
    for slot_index in range(1, N_SLOT):
        current = states[-1]
        for step in range(STEPS):
            padded = jnp.pad(current, ((0, 0), (1, 1), (1, 1)), mode="wrap")
            current = advance_slot(padded, winds[0, slot_index - 1], winds[1, slot_index - 1], mixing)
        states.append(current + forcing[slot_index])
    owner_blocks = N_TILE * N_OBS
    rows = N_OBS * CAP
    columns = CX * CY
    radiances = []
    for slot_index in range(N_SLOT):
        patch = states[slot_index].reshape(VL, N_TILE, CX, N_OBS, CY).transpose(1, 3, 0, 2, 4).reshape(owner_blocks, VL, columns)
        cells = observation_columns[:, slot_index].reshape(4, owner_blocks, rows)
        weights = obs_weights[:, slot_index].reshape(4, owner_blocks, rows)
        profile = jnp.zeros((owner_blocks, VL, rows), jnp.float32)
        for corner in range(4):
            index = jnp.broadcast_to(cells[corner][:, None, :], (owner_blocks, VL, rows)).astype(jnp.int32)
            picked = jnp.take_along_axis(patch, index, axis=2)
            profile = profile + weights[corner][:, None, :] * picked
        live = (jnp.arange(CAP, dtype=jnp.int32).reshape(1, 1, CAP) < obs_counts[slot_index][:, :, None]).astype(jnp.float32)
        profile = profile.reshape(N_TILE, N_OBS, VL, N_OBS, CAP) * live.reshape(N_TILE, N_OBS, 1, N_OBS, CAP)
        slot_output = jnp.einsum("ocv,tsvok->tocsk", jacobian[slot_index], profile, precision=lax.Precision.HIGHEST)
        radiances.append(slot_output.transpose(2, 0, 1, 3, 4).reshape(CHAN, owner_blocks * rows))
    return jnp.stack(states), jnp.stack(radiances)
```

```python
import functools

import jax
import jax.numpy as jnp
from jax import lax
from jax.experimental import pallas as pl
from jax.experimental.pallas import tpu as pltpu
from jax.sharding import Mesh
from jax.sharding import PartitionSpec as P

STEPS = 4
WIDE = 11
WINDOW = WIDE + 2 * STEPS
LANE_B = 32

mixing_rate = 0.15

SMEM = functools.partial(pl.BlockSpec, memory_space=pltpu.SMEM)
VMEM = functools.partial(pl.BlockSpec, memory_space=pltpu.VMEM)


def starts_of(width, planes):
    return [width * j // planes for j in range(planes + 1)]


def halves(x):
    high = x.astype(jnp.bfloat16)
    low = (x - high.astype(jnp.float32)).astype(jnp.bfloat16)
    return high, low


def cut_kernel(planes, odd_ref, forcing_ref, rates_ref, out_ref, turned):
    levels, width_x, width_y = forcing_ref.shape
    odd = odd_ref[0]
    for x in range(width_x):
        turned[:, x, :] = forcing_ref[:, x, :].T
    lane = lax.broadcasted_iota(jnp.int32, (width_x, rates_ref.shape[2]), 1)
    for j, start in enumerate(starts_of(width_y, planes)[:-1]):
        place = jnp.where(odd == 1, planes - 1 - j, j)
        out_ref[place, 0:WIDE] = turned[start : start + WIDE]
        whole = rates_ref.shape[2]
        east = pltpu.roll(rates_ref[0], (whole - start) % whole, 1)
        north = pltpu.roll(rates_ref[1], (whole + LANE_B - start) % whole, 1)
        both = jnp.where(lane < LANE_B, east, north)
        out_ref[place, WIDE] = both[:, :levels]


def spread_kernel(size_ref, first_ref, own_ref, up_ref, down_ref, rates_ref):
    nx, nz, rows, part, _ = first_ref.shape
    size = size_ref[0]
    for z in range(nz):
        for x in range(nx):
            at = (z * nx + x) * part
            own_ref[:, at : at + part, :] = first_ref[x, z, 0:WIDE]
            for s in range(rows - WIDE):
                rates_ref[s, at : at + part, :] = first_ref[x, z, WIDE + s]
    down_ref[...] = own_ref[0:STEPS]
    up_ref[...] = own_ref[pl.ds(size - STEPS, STEPS)]


def round_kernel(
    last, at_slot, size_ref, own_ref, low_ref, high_ref, rates_ref, forcing_ref, mix_ref, *rest
):
    if last:
        part_ref, ping, pong, east_rate, north_rate, table = rest
    else:
        next_ref, up_ref, down_ref, part_ref, ping, pong, east_rate, north_rate, table = rest
    size = size_ref[0]
    x_place = size_ref[1]
    whole_x = own_ref.shape[1]
    levels = own_ref.shape[2]
    ping[0:STEPS] = low_ref[...]
    ping[STEPS : STEPS + WIDE] = own_ref[...]
    ping[WINDOW - 1] = jnp.zeros((whole_x, levels), jnp.float32)
    ping[pl.ds(STEPS + size, STEPS)] = high_ref[...]
    for y in range(1, WINDOW - 1):
        east_rate[y] = jnp.broadcast_to(rates_ref[:, y : y + 1], (whole_x, levels))
        north_rate[y] = jnp.broadcast_to(
            rates_ref[:, LANE_B + y : LANE_B + y + 1], (whole_x, levels)
        )
    mix_high, mix_low = halves(mix_ref[...])
    table[0:levels, 0:levels] = mix_high
    table[levels:, 0:levels] = mix_high
    table[0:levels, levels:] = mix_low
    table[levels:, levels:] = mix_low
    bufs = (ping, pong)
    for step in range(STEPS):
        source, target = bufs[step % 2], bufs[(step + 1) % 2]
        first, end = step + 1, WINDOW - 1 - step
        pieces = []
        for y in range(first, end):
            centre = source[y]
            northern = source[y + 1]
            southern = source[y - 1]
            eastern = pltpu.roll(centre, whole_x - 1, 0)
            western = pltpu.roll(centre, 1, 0)
            z = centre + east_rate[y] * (eastern - western) + north_rate[y] * (northern - southern)
            z = z + mixing_rate * (
                (eastern + western) + (northern + southern) - 4.0 * centre
            )
            target[y] = z
        count = end - first
        z = target[first:end].reshape(count * whole_x, levels)
        high, low = halves(z)
        both = jnp.dot(
            jnp.concatenate([high, low], axis=1), table[...], preferred_element_type=jnp.float32
        )
        z = z + (both[:, :levels] + both[:, levels:])
        target[first:end] = z.reshape(count, whole_x, levels)
    result = bufs[STEPS % 2]
    nz, _, part, _ = part_ref.shape
    for z in range(nz):
        at = pl.multiple_of(z * (whole_x // nz) + x_place * part, part)
        part_ref[z] = result[STEPS : STEPS + WIDE, pl.ds(at, part), :]
    if not last:
        nx = forcing_ref.shape[0]
        for z in range(nz):
            for x in range(nx):
                at = (z * nx + x) * part
                next_ref[:, at : at + part, :] = (
                    result[STEPS : STEPS + WIDE, at : at + part, :] + forcing_ref[x, z, at_slot]
                )
        down_ref[...] = next_ref[0:STEPS]
        up_ref[...] = next_ref[pl.ds(size - STEPS, STEPS)]


def observe_kernel(
    planes, odd_ref, strips_ref, forcing_ref, cells_ref, weights_ref, state_ref, out_ref,
    turned, split,
):
    levels, width_x, width_y = forcing_ref.shape

    @pl.when(pl.program_id(0) == 0)
    def _():
        odd = odd_ref[0]
        starts = starts_of(width_y, planes)
        for j in range(planes):
            place = jnp.where(odd == 1, planes - 1 - j, j)
            turned[starts[j] : starts[j] + WIDE] = strips_ref[place]
        for x in range(width_x):
            value = turned[:, x, :].T + forcing_ref[:, x, :]
            state_ref[:, x, :] = value
            high, low = halves(value)
            split[0:levels, x * width_y : (x + 1) * width_y] = high
            split[levels:, x * width_y : (x + 1) * width_y] = low

    columns = width_x * width_y
    capacity = cells_ref.shape[1]
    column = lax.broadcasted_iota(jnp.int32, (columns, capacity), 0)
    table = jnp.zeros((columns, capacity), jnp.float32)
    for corner in range(cells_ref.shape[0]):
        cell = cells_ref[corner : corner + 1, :]
        weight = weights_ref[corner : corner + 1, :]
        table = table + jnp.where(column == cell, weight, 0.0)
    high, low = halves(table)
    both = jnp.dot(
        split[...], jnp.concatenate([high, low], axis=1), preferred_element_type=jnp.float32
    )
    out_ref[0] = both[:levels, :capacity] + (both[:levels, capacity:] + both[levels:, :capacity])


def channel_kernel(table_ref, profile_ref, out_ref):
    table_high, table_low = halves(table_ref[...])
    left = jnp.concatenate([table_high, table_low, table_high], axis=1)
    blocks, _, capacity = profile_ref.shape
    for block in range(blocks):
        high, low = halves(profile_ref[block])
        right = jnp.concatenate([high, high, low], axis=0)
        out_ref[:, block * capacity : (block + 1) * capacity] = jnp.dot(
            left, right, preferred_element_type=jnp.float32
        )


def f32(*shape):
    return jax.ShapeDtypeStruct(shape, jnp.float32)


def local(forcing, winds, mixing, observation_columns, obs_weights, obs_counts, jacobian):
    slots = lax.axis_size("slot")
    halves_z = lax.axis_size("zhi")
    parts_x = lax.axis_size("x")
    owners = lax.axis_size("obs")
    planes = slots * halves_z
    rounds = slots - 1
    block = forcing[0]
    levels, width_x, width_y = block.shape
    whole_x = width_x * parts_x * halves_z
    starts = starts_of(width_y, planes)

    place_o = lax.axis_index("obs")
    place_z = lax.axis_index("zhi") * slots + lax.axis_index("slot")
    odd = (place_o % 2).astype(jnp.int32)
    strip = jnp.where(odd == 1, planes - 1 - place_z, place_z)
    size = (width_y * (strip + 1)) // planes - (width_y * strip) // planes
    odd = odd.reshape(1)
    sizes = jnp.stack([size.astype(jnp.int32), lax.axis_index("x").astype(jnp.int32)])

    order = []
    for o in range(owners):
        along = range(planes) if o % 2 == 0 else range(planes - 1, -1, -1)
        order += [((z % slots) * halves_z + z // slots) * owners + o for z in along]
    upward = [(order[i - 1], order[i]) for i in range(len(order))]
    downward = [(target, source) for source, target in upward]
    chain = ("slot", "zhi", "obs")

    rates = winds[:, 0]
    ring = [(i, (i + 1) % owners) for i in range(owners)]
    back = [(target, source) for source, target in ring]
    rates_low = lax.ppermute(rates[:, :, width_y - STEPS :], "obs", ring)
    rates_high = lax.ppermute(rates[:, :, :STEPS], "obs", back)
    rates = jnp.concatenate(
        [rates_low, rates, rates_high, jnp.zeros((2, width_x, width_y - 2 * STEPS), jnp.float32)],
        axis=2,
    )

    cut = pl.pallas_call(
        functools.partial(cut_kernel, planes),
        out_shape=f32(planes, WIDE + 1, width_x, levels),
        in_specs=[SMEM(), VMEM(), VMEM()],
        out_specs=VMEM(),
        scratch_shapes=[pltpu.VMEM((width_y, width_x, levels), jnp.float32)],
        cost_estimate=pl.CostEstimate(flops=4000000, bytes_accessed=1100000, transcendentals=0),
        name="cut",
    )(odd, block, rates)
    strips = lax.all_to_all(cut, ("zhi", "slot"), 0, 0, tiled=True)
    strips = strips.reshape(halves_z, slots, WIDE + 1, width_x, levels)
    first = jnp.concatenate(
        [strips[:, 0, :WIDE], strips[:, :rounds, WIDE]], axis=1
    )
    later = strips[:, 1:rounds, :WIDE]
    first = lax.all_to_all(
        jnp.broadcast_to(first, (parts_x,) + first.shape), "x", 0, 0, tiled=True
    ).reshape((parts_x,) + first.shape)
    later = lax.all_to_all(
        jnp.broadcast_to(later, (parts_x,) + later.shape), "x", 0, 0, tiled=True
    ).reshape((parts_x,) + later.shape)

    strip_shape = f32(WIDE, whole_x, levels)
    edge_shape = f32(STEPS, whole_x, levels)
    part_shape = f32(halves_z, WIDE, width_x, levels)
    own, up, down, rates = pl.pallas_call(
        spread_kernel,
        out_shape=(strip_shape, edge_shape, edge_shape, f32(rounds, whole_x, levels)),
        in_specs=[SMEM(), VMEM()],
        out_specs=(VMEM(),) * 4,
        cost_estimate=pl.CostEstimate(flops=1000000, bytes_accessed=1500000, transcendentals=0),
        name="spread",
    )(sizes, first)

    turned_mixing = mixing.T
    window = pltpu.VMEM((WINDOW, whole_x, levels), jnp.float32)
    kept = []
    for index in range(rounds):
        last = index == rounds - 1
        low = lax.ppermute(up, chain, upward)
        high = lax.ppermute(down, chain, downward)
        shapes = (part_shape,) if last else (strip_shape, edge_shape, edge_shape, part_shape)
        results = pl.pallas_call(
            functools.partial(round_kernel, last, min(index, rounds - 2)),
            out_shape=shapes,
            in_specs=[SMEM()] + [VMEM()] * 6,
            out_specs=(VMEM(),) * len(shapes),
            scratch_shapes=[window] * 4 + [pltpu.VMEM((2 * levels, 2 * levels), jnp.bfloat16)],
            cost_estimate=pl.CostEstimate(
                flops=400000000, bytes_accessed=3000000, transcendentals=0
            ),
            name="round",
        )(sizes, own, low, high, rates[index], later, turned_mixing)
        kept.append(results[-1])
        if not last:
            own, up, down = results[:3]

    home = jnp.stack([jnp.zeros_like(kept[0])] + kept, axis=1)
    home = home.reshape(planes, WIDE, width_x, levels)
    home = lax.all_to_all(home, ("zhi", "slot"), 0, 0, tiled=True)

    cells = observation_columns[:, 0]
    weights = obs_weights[:, 0]
    points, row_count = cells.shape
    capacity = row_count // owners
    live = lax.broadcasted_iota(jnp.int32, (owners, capacity), 1) < obs_counts[0, 0][:, None]
    weights = jnp.where(live.reshape(1, row_count), weights, 0.0)

    columns = width_x * width_y
    state, profile = pl.pallas_call(
        functools.partial(observe_kernel, planes),
        out_shape=(f32(levels, width_x, width_y), f32(owners, levels, capacity)),
        grid=(owners,),
        in_specs=[
            SMEM(),
            pl.BlockSpec((planes, WIDE, width_x, levels), lambda q: (0, 0, 0, 0)),
            pl.BlockSpec((levels, width_x, width_y), lambda q: (0, 0, 0)),
            pl.BlockSpec((points, capacity), lambda q: (0, q)),
            pl.BlockSpec((points, capacity), lambda q: (0, q)),
        ],
        out_specs=(
            pl.BlockSpec((levels, width_x, width_y), lambda q: (0, 0, 0)),
            pl.BlockSpec((1, levels, capacity), lambda q: (q, 0, 0)),
        ),
        scratch_shapes=[
            pltpu.VMEM((width_y, width_x, levels), jnp.float32),
            pltpu.VMEM((2 * levels, columns), jnp.bfloat16),
        ],
        cost_estimate=pl.CostEstimate(
            flops=2000000000, bytes_accessed=3000000, transcendentals=0
        ),
        name="observe",
    )(odd, home, block, cells, weights)

    profile = lax.all_to_all(profile, "obs", 0, 0, tiled=True)
    channels = jacobian.shape[2]
    group = 4
    radiance = pl.pallas_call(
        channel_kernel,
        out_shape=f32(channels, row_count),
        grid=(owners // group,),
        in_specs=[
            pl.BlockSpec((channels, levels), lambda q: (0, 0)),
            pl.BlockSpec((group, levels, capacity), lambda q: (q, 0, 0)),
        ],
        out_specs=pl.BlockSpec((channels, group * capacity), lambda q: (0, q)),
        cost_estimate=pl.CostEstimate(
            flops=200000000, bytes_accessed=2200000, transcendentals=0
        ),
        name="channel",
    )(jacobian[0, 0], profile)
    return (state[None], radiance[None])


def solution(mesh):
    slots, tiles, owners = (mesh.shape[name] for name in ("slot", "tile", "obs"))
    fine = Mesh(
        mesh.devices.reshape(slots, 2, tiles // 2, owners), ("slot", "zhi", "x", "obs")
    )
    tile = ("zhi", "x")
    return jax.shard_map(
        local,
        mesh=fine,
        in_specs=(
            P("slot", None, tile, "obs"),
            P(None, "slot", tile, "obs"),
            P(),
            P(None, "slot", tile + ("obs",)),
            P(None, "slot", tile + ("obs",)),
            P("slot", tile + ("obs",), None),
            P("slot", "obs", None, None),
        ),
        out_specs=(P("slot", None, tile, "obs"), P("slot", None, tile + ("obs",))),
        check_vma=False,
    )
```

```python
import functools

import jax
import jax.numpy as jnp
from jax import lax
from jax.experimental import pallas as pl
from jax.experimental.pallas import tpu as pltpu
from jax.sharding import Mesh
from jax.sharding import PartitionSpec as P

STEPS = 4
REACH = 2 * STEPS
WIDE = 11
LANE_B = 32

mixing_rate = 0.15

SMEM = functools.partial(pl.BlockSpec, memory_space=pltpu.SMEM)
VMEM = functools.partial(pl.BlockSpec, memory_space=pltpu.VMEM)


def params(mebibytes):
    return pltpu.CompilerParams(vmem_limit_bytes=mebibytes << 20)


def cost(flops, moved):
    return pl.CostEstimate(flops=flops, bytes_accessed=moved, transcendentals=0)


def starts_of(width, planes):
    return [width * j // planes for j in range(planes + 1)]


def halves(x):
    high = x.astype(jnp.bfloat16)
    low = (x - high.astype(jnp.float32)).astype(jnp.bfloat16)
    return high, low


def cut_kernel(planes, odd_ref, forcing_ref, rates_ref, around_ref, out_ref, turned):
    levels, width_x, width_y = forcing_ref.shape
    odd = odd_ref[0]
    for x in range(width_x):
        turned[:, x, :] = forcing_ref[:, x, :].T
    whole = 2 * width_y
    lane = lax.broadcasted_iota(jnp.int32, (width_x, whole), 1)
    east_all = jnp.concatenate([rates_ref[0], around_ref[0]], axis=1)
    north_all = jnp.concatenate([rates_ref[1], around_ref[1]], axis=1)
    for j, start in enumerate(starts_of(width_y, planes)[:-1]):
        place = jnp.where(odd == 1, planes - 1 - j, j)
        out_ref[place, 0:WIDE] = turned[start : start + WIDE]
        offset = REACH - start
        east = pltpu.roll(east_all, (whole + offset) % whole, 1)
        north = pltpu.roll(north_all, (whole + LANE_B + offset) % whole, 1)
        both = jnp.where(lane < LANE_B, east, north)
        out_ref[place, WIDE] = both[:, :levels]


def edges(size, up_ref, down_ref, state_ref, forcing_ref=None):
    depth = REACH if forcing_ref is not None else STEPS
    down_ref[0:depth] = state_ref[0:depth]
    up_ref[0:depth] = state_ref[pl.ds(size - depth, depth)]
    if forcing_ref is not None:
        down_ref[depth:] = forcing_ref[0:STEPS]
        up_ref[depth:] = forcing_ref[pl.ds(size - STEPS, STEPS)]


def spread_kernel(size_ref, first_ref, own_ref, next_ref, up_ref, down_ref, rates_ref):
    nx, nz, rows, part, _ = first_ref.shape
    for z in range(nz):
        for x in range(nx):
            at = (z * nx + x) * part
            own_ref[:, at : at + part, :] = first_ref[x, z, 0:WIDE]
            next_ref[:, at : at + part, :] = first_ref[x, z, WIDE : 2 * WIDE]
            for s in range(rows - 2 * WIDE):
                rates_ref[s, at : at + part, :] = first_ref[x, z, 2 * WIDE + s]
    edges(size_ref[0], up_ref, down_ref, own_ref, next_ref)


def fill_window(window, reach, size, own, low, high):
    window[0:reach] = low
    window[reach : reach + WIDE] = own
    window[reach + WIDE + reach - 1] = jnp.zeros(window.shape[1:], jnp.float32)
    window[pl.ds(reach + size, reach)] = high


def fill_table(table, mix_ref):
    levels = mix_ref.shape[0]
    mix_high, mix_low = halves(mix_ref[...])
    table[0:levels] = mix_high
    table[levels : 2 * levels] = mix_high
    table[2 * levels :] = mix_low


def advance(bufs, first, end, lane, rate, rate_refs, table):
    _, whole_x, levels = bufs[0].shape
    to_east, to_west, to_north, to_south = rate_refs
    shape = (whole_x, levels)
    for y in range(first + 1, end - 1):
        east = jnp.broadcast_to(rate[:, lane + y : lane + y + 1], shape)
        north = jnp.broadcast_to(rate[:, LANE_B + lane + y : LANE_B + lane + y + 1], shape)
        to_east[y] = mixing_rate + east
        to_west[y] = mixing_rate - east
        to_north[y] = mixing_rate + north
        to_south[y] = mixing_rate - north
    for step in range(STEPS):
        source, target = bufs[step % 2], bufs[(step + 1) % 2]
        low, high = first + step + 1, end - step - 1
        for y in range(low, high):
            centre = source[y]
            eastern = pltpu.roll(centre, whole_x - 1, 0)
            western = pltpu.roll(centre, 1, 0)
            across = to_east[y] * eastern + to_west[y] * western
            along = to_north[y] * source[y + 1] + to_south[y] * source[y - 1]
            target[y] = (1.0 - 4.0 * mixing_rate) * centre + (across + along)
        count = high - low
        z = target[low:high].reshape(count * whole_x, levels)
        z_high, z_low = halves(z)
        z = z + jnp.dot(
            jnp.concatenate([z_high, z_low, z_high], axis=1),
            table[...],
            preferred_element_type=jnp.float32,
        )
        target[low:high] = z.reshape(count, whole_x, levels)


def take_part(part_ref, window, reach, x_place):
    nz, _, part, _ = part_ref.shape
    whole_x = window.shape[1]
    for z in range(nz):
        at = pl.multiple_of(z * (whole_x // nz) + x_place * part, part)
        part_ref[z] = window[reach : reach + WIDE, pl.ds(at, part), :]


def gather_x(out_ref, later_ref, index):
    nx, nz, _, _, part, _ = later_ref.shape
    for z in range(nz):
        for x in range(nx):
            at = (z * nx + x) * part
            out_ref[:, at : at + part, :] = later_ref[x, z, index]


def two_slots(size_ref, own_ref, mid_ref, low_ref, high_ref, rates, mix_ref, parts, scratch):
    ping, pong, force, table = scratch[:4]
    coefficients = scratch[4:]
    size, x_place = size_ref[0], size_ref[1]
    fill_window(ping, REACH, size, own_ref[...], low_ref[0:REACH], high_ref[0:REACH])
    fill_window(force, STEPS, size, mid_ref[...], low_ref[REACH:], high_ref[REACH:])
    fill_table(table, mix_ref)
    rows = WIDE + 2 * REACH
    advance((ping, pong), 0, rows, 0, rates[0], coefficients, table)
    take_part(parts[0], ping, REACH, x_place)
    ping[STEPS : rows - STEPS] = ping[STEPS : rows - STEPS] + force[...]
    advance((ping, pong), STEPS, rows - STEPS, 0, rates[1], coefficients, table)
    take_part(parts[1], ping, REACH, x_place)
    return ping[REACH : REACH + WIDE]


def early_kernel(
    size_ref, own_ref, mid_ref, low_ref, high_ref, rates_ref, mix_ref, later_ref,
    next_ref, mid_next_ref, end_next_ref, up_ref, down_ref, part_a, part_b, *scratch,
):
    gather_x(next_ref, later_ref, 0)
    gather_x(mid_next_ref, later_ref, 1)
    gather_x(end_next_ref, later_ref, 2)
    moved = two_slots(
        size_ref, own_ref, mid_ref, low_ref, high_ref, (rates_ref.at[0], rates_ref.at[1]),
        mix_ref, (part_a, part_b), scratch,
    )
    next_ref[...] = next_ref[...] + moved
    edges(size_ref[0], up_ref, down_ref, next_ref, mid_next_ref)


def middle_kernel(
    size_ref, own_ref, mid_ref, low_ref, high_ref, rates_ref, mix_ref, end_ref,
    next_ref, up_ref, down_ref, part_a, part_b, *scratch,
):
    moved = two_slots(
        size_ref, own_ref, mid_ref, low_ref, high_ref, (rates_ref.at[2], rates_ref.at[3]),
        mix_ref, (part_a, part_b), scratch,
    )
    next_ref[...] = end_ref[...] + moved
    edges(size_ref[0], up_ref, down_ref, next_ref)


def late_kernel(
    size_ref, own_ref, low_ref, high_ref, rates_ref, mix_ref, *rest
):
    kept, home_ref, (ping, pong, table) = rest[:4], rest[4], rest[5:8]
    coefficients = rest[8:]
    fill_window(ping, STEPS, size_ref[0], own_ref[...], low_ref[...], high_ref[...])
    fill_table(table, mix_ref)
    nz = home_ref.shape[0]
    home_ref[:, 0] = jnp.zeros_like(kept[0])
    for index, part in enumerate(kept):
        home_ref[:, index + 1] = part[...]
    advance(
        (ping, pong), 0, WIDE + 2 * STEPS, STEPS, rates_ref.at[4], coefficients, table
    )
    take_part(home_ref.at[:, 5], ping, STEPS, size_ref[1])


def table_kernel(cells_ref, weights_ref, out_ref):
    _, columns, wide = out_ref.shape
    capacity = wide // 2
    column = lax.broadcasted_iota(jnp.int32, (columns, capacity), 0)
    for owner in range(out_ref.shape[0]):
        at = slice(owner * capacity, (owner + 1) * capacity)
        table = None
        for corner in range(cells_ref.shape[0]):
            cell = cells_ref[corner : corner + 1, at]
            weight = weights_ref[corner : corner + 1, at]
            term = jnp.where(column == cell, weight, 0.0)
            table = term if table is None else table + term
        high, low = halves(table)
        out_ref[owner, :, :capacity] = high
        out_ref[owner, :, capacity:] = low


def observe_kernel(
    planes, odd_ref, strips_ref, forcing_ref, table_ref, state_ref, out_ref, turned, split
):
    levels, width_x, width_y = forcing_ref.shape

    @pl.when(pl.program_id(0) == 0)
    def _():
        odd = odd_ref[0]
        starts = starts_of(width_y, planes)
        for j in range(planes):
            place = jnp.where(odd == 1, planes - 1 - j, j)
            turned[starts[j] : starts[j] + WIDE] = strips_ref[place]
        for x in range(width_x):
            value = turned[:, x, :].T + forcing_ref[:, x, :]
            state_ref[:, x, :] = value
            high, low = halves(value)
            split[0:levels, x * width_y : (x + 1) * width_y] = high
            split[levels:, x * width_y : (x + 1) * width_y] = low

    capacity = out_ref.shape[2]
    for owner in range(out_ref.shape[0]):
        both = jnp.dot(split[...], table_ref[owner], preferred_element_type=jnp.float32)
        out_ref[owner] = both[:levels, :capacity] + (
            both[:levels, capacity:] + both[levels:, :capacity]
        )


def channel_kernel(table_ref, profile_ref, out_ref):
    table_high, table_low = halves(table_ref[...])
    left = jnp.concatenate([table_high, table_low, table_high], axis=1)
    blocks, _, capacity = profile_ref.shape
    group = 4
    for block in range(0, blocks, group):
        value = jnp.concatenate([profile_ref[block + i] for i in range(group)], axis=1)
        high, low = halves(value)
        right = jnp.concatenate([high, high, low], axis=0)
        out_ref[:, block * capacity : (block + group) * capacity] = jnp.dot(
            left, right, preferred_element_type=jnp.float32
        )


def f32(*shape):
    return jax.ShapeDtypeStruct(shape, jnp.float32)


def local(forcing, winds, mixing, observation_columns, obs_weights, obs_counts, jacobian):
    slots = lax.axis_size("slot")
    halves_z = lax.axis_size("zhi")
    parts_x = lax.axis_size("x")
    owners = lax.axis_size("obs")
    planes = slots * halves_z
    rounds = slots - 1
    block = forcing[0]
    levels, width_x, width_y = block.shape
    whole_x = width_x * parts_x * halves_z
    starts = starts_of(width_y, planes)

    place_o = lax.axis_index("obs")
    place_z = lax.axis_index("zhi") * slots + lax.axis_index("slot")
    odd = (place_o % 2).astype(jnp.int32)
    strip = jnp.where(odd == 1, planes - 1 - place_z, place_z)
    size = (width_y * (strip + 1)) // planes - (width_y * strip) // planes
    odd = odd.reshape(1)
    sizes = jnp.stack([size.astype(jnp.int32), lax.axis_index("x").astype(jnp.int32)])

    order = []
    for o in range(owners):
        along = range(planes) if o % 2 == 0 else range(planes - 1, -1, -1)
        order += [((z % slots) * halves_z + z // slots) * owners + o for z in along]
    upward = [(order[i - 1], order[i]) for i in range(len(order))]
    downward = [(target, source) for source, target in upward]
    chain = ("slot", "zhi", "obs")

    rates = winds[:, 0]
    ring = [(i, (i + 1) % owners) for i in range(owners)]
    back = [(target, source) for source, target in ring]
    rates_low = lax.ppermute(rates[:, :, width_y - REACH :], "obs", ring)
    rates_high = lax.ppermute(rates[:, :, :REACH], "obs", back)
    around = jnp.concatenate(
        [rates_high, jnp.zeros((2, width_x, width_y - 2 * REACH), jnp.float32), rates_low], axis=2
    )

    cut = pl.pallas_call(
        functools.partial(cut_kernel, planes),
        out_shape=f32(planes, WIDE + 1, width_x, levels),
        in_specs=[SMEM()] + [VMEM()] * 3,
        out_specs=VMEM(),
        scratch_shapes=[pltpu.VMEM((width_y, width_x, levels), jnp.float32)],
        compiler_params=params(8),
        cost_estimate=cost(4000000, 1100000),
        name="cut",
    )(odd, block, rates, around)
    strips = lax.all_to_all(cut, ("zhi", "slot"), 0, 0, tiled=True)
    strips = strips.reshape(halves_z, slots, WIDE + 1, width_x, levels)
    first = jnp.concatenate(
        [strips[:, 0, :WIDE], strips[:, 1, :WIDE], strips[:, :rounds, WIDE]], axis=1
    )
    later = strips[:, 2:rounds, :WIDE]
    first = lax.all_to_all(
        jnp.broadcast_to(first, (parts_x,) + first.shape), "x", 0, 0, tiled=True
    ).reshape((parts_x,) + first.shape)
    later = lax.all_to_all(
        jnp.broadcast_to(later, (parts_x,) + later.shape), "x", 0, 0, tiled=True
    ).reshape((parts_x,) + later.shape)

    strip = f32(WIDE, whole_x, levels)
    far = pltpu.HBM((WIDE, whole_x, levels), jnp.float32)
    edge = f32(REACH + STEPS, whole_x, levels)
    last_edge = f32(STEPS, whole_x, levels)
    part = f32(halves_z, WIDE, width_x, levels)
    own, mid, up, down, rates = pl.pallas_call(
        spread_kernel,
        out_shape=(far, far, edge, edge, f32(rounds, whole_x, levels)),
        in_specs=[SMEM(), VMEM()],
        out_specs=(VMEM(),) * 5,
        compiler_params=params(8),
        cost_estimate=cost(1000000, 2500000),
        name="spread",
    )(sizes, first)

    turned_mixing = mixing.T
    table = pltpu.VMEM((3 * levels, levels), jnp.bfloat16)

    def window(rows):
        return pltpu.VMEM((rows, whole_x, levels), jnp.float32)

    long = WIDE + 2 * REACH
    short = WIDE + 2 * STEPS
    long_scratch = [window(long)] * 2 + [window(short), table] + [window(long)] * 4
    short_scratch = [window(short)] * 2 + [table] + [window(short)] * 4

    low = lax.ppermute(up, chain, upward)
    high = lax.ppermute(down, chain, downward)
    own, mid = (pltpu.with_memory_space_constraint(x, pltpu.HBM) for x in (own, mid))
    own, mid, end, up, down, *kept = pl.pallas_call(
        early_kernel,
        out_shape=(strip, strip, strip, edge, edge, part, part),
        in_specs=[SMEM()] + [VMEM()] * 7,
        out_specs=(VMEM(),) * 7,
        scratch_shapes=long_scratch,
        compiler_params=params(24),
        cost_estimate=cost(900000000, 4000000),
        name="early",
    )(sizes, own, mid, low, high, rates, turned_mixing, later)
    low = lax.ppermute(up, chain, upward)
    high = lax.ppermute(down, chain, downward)
    own, up, down, *kept[2:] = pl.pallas_call(
        middle_kernel,
        out_shape=(strip, last_edge, last_edge, part, part),
        in_specs=[SMEM()] + [VMEM()] * 7,
        out_specs=(VMEM(),) * 5,
        scratch_shapes=long_scratch,
        compiler_params=params(24),
        cost_estimate=cost(900000000, 4000000),
        name="middle",
    )(sizes, own, mid, low, high, rates, turned_mixing, end)
    low = lax.ppermute(up, chain, upward)
    high = lax.ppermute(down, chain, downward)
    home = pl.pallas_call(
        late_kernel,
        out_shape=f32(halves_z, slots, WIDE, width_x, levels),
        in_specs=[SMEM()] + [VMEM()] * 9,
        out_specs=VMEM(),
        scratch_shapes=short_scratch,
        compiler_params=params(24),
        cost_estimate=cost(400000000, 3000000),
        name="late",
    )(sizes, own, low, high, rates, turned_mixing, *kept)

    cells = observation_columns[:, 0]
    points, row_count = cells.shape
    capacity = row_count // owners
    live = lax.broadcasted_iota(jnp.int32, (owners, capacity), 1) < obs_counts[0, 0][:, None]
    weights = jnp.where(live.reshape(1, row_count), obs_weights[:, 0], 0.0)
    home, weights = lax.optimization_barrier((home, weights))
    home = home.reshape(planes, WIDE, width_x, levels)
    home = lax.all_to_all(home, ("zhi", "slot"), 0, 0, tiled=True)

    columns = width_x * width_y
    group = 2
    tables = pl.pallas_call(
        table_kernel,
        out_shape=pltpu.HBM((owners, columns, 2 * capacity), jnp.bfloat16),
        grid=(owners // group,),
        in_specs=[pl.BlockSpec((points, group * capacity), lambda q: (0, q))] * 2,
        out_specs=pl.BlockSpec((group, columns, 2 * capacity), lambda q: (q, 0, 0)),
        compiler_params=params(20),
        cost_estimate=cost(1000000000, 8500000),
        name="table",
    )(cells, weights)
    tables = pltpu.with_memory_space_constraint(tables, pltpu.HBM)
    state, profile = pl.pallas_call(
        functools.partial(observe_kernel, planes),
        out_shape=(f32(levels, width_x, width_y), f32(owners, levels, capacity)),
        grid=(owners // group,),
        in_specs=[
            SMEM(),
            pl.BlockSpec((planes, WIDE, width_x, levels), lambda q: (0, 0, 0, 0)),
            pl.BlockSpec((levels, width_x, width_y), lambda q: (0, 0, 0)),
            pl.BlockSpec((group, columns, 2 * capacity), lambda q: (q, 0, 0)),
        ],
        out_specs=(
            pl.BlockSpec((levels, width_x, width_y), lambda q: (0, 0, 0)),
            pl.BlockSpec((group, levels, capacity), lambda q: (q, 0, 0)),
        ),
        scratch_shapes=[
            pltpu.VMEM((width_y, width_x, levels), jnp.float32),
            pltpu.VMEM((2 * levels, columns), jnp.bfloat16),
        ],
        compiler_params=params(20),
        cost_estimate=cost(2000000000, 11000000),
        name="observe",
    )(odd, home, block, tables)

    profile = lax.all_to_all(profile, "obs", 0, 0, tiled=True)
    channels = jacobian.shape[2]
    radiance = pl.pallas_call(
        channel_kernel,
        out_shape=f32(channels, row_count),
        in_specs=[VMEM()] * 2,
        out_specs=VMEM(),
        compiler_params=params(12),
        cost_estimate=cost(200000000, 2200000),
        name="channel",
    )(jacobian[0, 0], profile)
    return (state[None], radiance[None])


def solution(mesh):
    slots, tiles, owners = (mesh.shape[name] for name in ("slot", "tile", "obs"))
    fine = Mesh(
        mesh.devices.reshape(slots, 2, tiles // 2, owners), ("slot", "zhi", "x", "obs")
    )
    tile = ("zhi", "x")
    return jax.shard_map(
        local,
        mesh=fine,
        in_specs=(
            P("slot", None, tile, "obs"),
            P(None, "slot", tile, "obs"),
            P(),
            P(None, "slot", tile + ("obs",)),
            P(None, "slot", tile + ("obs",)),
            P("slot", tile + ("obs",), None),
            P("slot", "obs", None, None),
        ),
        out_specs=(P("slot", None, tile, "obs"), P("slot", None, tile + ("obs",))),
        check_vma=False,
    )
```

```python
import functools

import jax
import jax.numpy as jnp
from jax import lax
from jax.experimental import pallas as pl
from jax.experimental.pallas import tpu as pltpu
from jax.sharding import Mesh
from jax.sharding import PartitionSpec as P

STEPS = 4
REACH = 2 * STEPS
WIDE = 11
LANE_B = 32

mixing_rate = 0.15

SMEM = functools.partial(pl.BlockSpec, memory_space=pltpu.SMEM)
VMEM = functools.partial(pl.BlockSpec, memory_space=pltpu.VMEM)


def params(mebibytes):
    return pltpu.CompilerParams(vmem_limit_bytes=mebibytes << 20)


def cost(flops, moved):
    return pl.CostEstimate(flops=flops, bytes_accessed=moved, transcendentals=0)


def starts_of(width, planes):
    return [width * j // planes for j in range(planes + 1)]


def halves(x):
    high = x.astype(jnp.bfloat16)
    low = (x - high.astype(jnp.float32)).astype(jnp.bfloat16)
    return high, low


def cut_kernel(planes, odd_ref, forcing_ref, rates_ref, out_ref, turned):
    levels, width_x, width_y = forcing_ref.shape
    odd = odd_ref[0]
    for x in range(width_x):
        turned[:, x, :] = forcing_ref[:, x, :].T
    lane = lax.broadcasted_iota(jnp.int32, (width_x, width_y), 1)
    for j, start in enumerate(starts_of(width_y, planes)[:-1]):
        place = jnp.where(odd == 1, planes - 1 - j, j)
        out_ref[place, 0:WIDE] = turned[start : start + WIDE]
        east = pltpu.roll(rates_ref[0], (width_y - start) % width_y, 1)
        north = pltpu.roll(rates_ref[1], (width_y + WIDE - start) % width_y, 1)
        both = jnp.where(lane < WIDE, east, north)
        out_ref[place, WIDE] = jnp.where(lane < 2 * WIDE, both, 0.0)


def edges(size, up_ref, down_ref, state_ref, forcing_ref=None):
    depth = REACH if forcing_ref is not None else STEPS
    down_ref[0:depth] = state_ref[0:depth]
    up_ref[0:depth] = state_ref[pl.ds(size - depth, depth)]
    if forcing_ref is not None:
        down_ref[depth : depth + STEPS] = forcing_ref[0:STEPS]
        up_ref[depth : depth + STEPS] = forcing_ref[pl.ds(size - STEPS, STEPS)]


def spread_kernel(size_ref, first_ref, own_ref, next_ref, up_ref, down_ref, rates_ref):
    nx, nz, rows, part, _ = first_ref.shape
    for z in range(nz):
        for x in range(nx):
            at = (z * nx + x) * part
            own_ref[:, at : at + part, :] = first_ref[x, z, 0:WIDE]
            next_ref[:, at : at + part, :] = first_ref[x, z, WIDE : 2 * WIDE]
            packed = first_ref[x, z, 2 * WIDE]
            for s in range(1, rows - 2 * WIDE):
                packed = packed + pltpu.roll(first_ref[x, z, 2 * WIDE + s], 2 * WIDE * s, 1)
            rates_ref[at : at + part, :] = packed
    edges(size_ref[0], up_ref, down_ref, own_ref, next_ref)
    down_ref[REACH + STEPS] = rates_ref[...]
    up_ref[REACH + STEPS] = rates_ref[...]


def widen_rates(out_ref, size_ref, own, low, high):
    shape = own.shape
    lanes = shape[1]
    size, size_low = size_ref[0], size_ref[2]
    lane = lax.broadcasted_iota(jnp.int32, shape, 1)
    first = lane < LANE_B
    place = jnp.where(first, lane, lane - LANE_B)

    def moved(value, base, shift):
        east = pltpu.roll(value, lax.rem(shift - base + 2 * lanes, lanes), 1)
        north = pltpu.roll(value, lax.rem(shift + LANE_B - WIDE - base + 2 * lanes, lanes), 1)
        return jnp.where(first, east, north)

    for s in range(out_ref.shape[0]):
        base = jnp.int32(2 * WIDE * s)
        below = moved(low, base, REACH - size_low)
        within = moved(own, base, jnp.int32(REACH))
        above = moved(high, base, REACH + size)
        out_ref[s] = jnp.where(
            place < REACH, below, jnp.where(place < REACH + size, within, above)
        )


def fill_window(window, reach, size, own, low, high):
    window[0:reach] = low
    window[reach : reach + WIDE] = own
    window[reach + WIDE + reach - 1] = jnp.zeros(window.shape[1:], jnp.float32)
    window[pl.ds(reach + size, reach)] = high


def fill_table(table, mix_ref):
    levels = mix_ref.shape[0]
    mix_high, mix_low = halves(mix_ref[...])
    table[0:levels] = mix_high
    table[levels : 2 * levels] = mix_high
    table[2 * levels :] = mix_low


def advance(bufs, first, end, lane, rate, rate_refs, table):
    _, whole_x, levels = bufs[0].shape
    to_east, to_west, to_north, to_south = rate_refs
    shape = (whole_x, levels)
    for y in range(first + 1, end - 1):
        east = jnp.broadcast_to(rate[:, lane + y : lane + y + 1], shape)
        north = jnp.broadcast_to(rate[:, LANE_B + lane + y : LANE_B + lane + y + 1], shape)
        to_east[y] = mixing_rate + east
        to_west[y] = mixing_rate - east
        to_north[y] = mixing_rate + north
        to_south[y] = mixing_rate - north
    for step in range(STEPS):
        source, target = bufs[step % 2], bufs[(step + 1) % 2]
        low, high = first + step + 1, end - step - 1
        for y in range(low, high):
            centre = source[y]
            eastern = pltpu.roll(centre, whole_x - 1, 0)
            western = pltpu.roll(centre, 1, 0)
            across = to_east[y] * eastern + to_west[y] * western
            along = to_north[y] * source[y + 1] + to_south[y] * source[y - 1]
            target[y] = (1.0 - 4.0 * mixing_rate) * centre + (across + along)
        count = high - low
        z = target[low:high].reshape(count * whole_x, levels)
        z_high, z_low = halves(z)
        z = z + jnp.dot(
            jnp.concatenate([z_high, z_low, z_high], axis=1),
            table[...],
            preferred_element_type=jnp.float32,
        )
        target[low:high] = z.reshape(count, whole_x, levels)


def take_part(part_ref, window, reach, x_place):
    nz, _, part, _ = part_ref.shape
    whole_x = window.shape[1]
    for z in range(nz):
        at = pl.multiple_of(z * (whole_x // nz) + x_place * part, part)
        part_ref[z] = window[reach : reach + WIDE, pl.ds(at, part), :]


def gather_x(out_ref, later_ref, index):
    nx, nz, _, _, part, _ = later_ref.shape
    for z in range(nz):
        for x in range(nx):
            at = (z * nx + x) * part
            out_ref[:, at : at + part, :] = later_ref[x, z, index]


def two_slots(size_ref, own_ref, mid_ref, low_ref, high_ref, rates, mix_ref, parts, scratch):
    ping, pong, force, table = scratch[:4]
    coefficients = scratch[4:]
    size, x_place = size_ref[0], size_ref[1]
    fill_window(ping, REACH, size, own_ref[...], low_ref[0:REACH], high_ref[0:REACH])
    fill_window(
        force, STEPS, size, mid_ref[...], low_ref[REACH : REACH + STEPS],
        high_ref[REACH : REACH + STEPS],
    )
    fill_table(table, mix_ref)
    rows = WIDE + 2 * REACH
    advance((ping, pong), 0, rows, 0, rates[0], coefficients, table)
    take_part(parts[0], ping, REACH, x_place)
    ping[STEPS : rows - STEPS] = ping[STEPS : rows - STEPS] + force[...]
    advance((ping, pong), STEPS, rows - STEPS, 0, rates[1], coefficients, table)
    take_part(parts[1], ping, REACH, x_place)
    return ping[REACH : REACH + WIDE]


def early_kernel(
    size_ref, own_ref, mid_ref, low_ref, high_ref, packed_ref, mix_ref, later_ref,
    next_ref, mid_next_ref, end_next_ref, up_ref, down_ref, part_a, part_b, rates_ref, *scratch,
):
    at = REACH + STEPS
    widen_rates(rates_ref, size_ref, packed_ref[...], low_ref[at], high_ref[at])
    gather_x(next_ref, later_ref, 0)
    gather_x(mid_next_ref, later_ref, 1)
    gather_x(end_next_ref, later_ref, 2)
    moved = two_slots(
        size_ref, own_ref, mid_ref, low_ref, high_ref, (rates_ref.at[0], rates_ref.at[1]),
        mix_ref, (part_a, part_b), scratch,
    )
    next_ref[...] = next_ref[...] + moved
    edges(size_ref[0], up_ref, down_ref, next_ref, mid_next_ref)


def middle_kernel(
    size_ref, own_ref, mid_ref, low_ref, high_ref, rates_ref, mix_ref, end_ref,
    next_ref, up_ref, down_ref, part_a, part_b, *scratch,
):
    moved = two_slots(
        size_ref, own_ref, mid_ref, low_ref, high_ref, (rates_ref.at[2], rates_ref.at[3]),
        mix_ref, (part_a, part_b), scratch,
    )
    next_ref[...] = end_ref[...] + moved
    edges(size_ref[0], up_ref, down_ref, next_ref)


def late_kernel(
    size_ref, own_ref, low_ref, high_ref, rates_ref, mix_ref, *rest
):
    kept, home_ref, (ping, pong, table) = rest[:4], rest[4], rest[5:8]
    coefficients = rest[8:]
    fill_window(ping, STEPS, size_ref[0], own_ref[...], low_ref[...], high_ref[...])
    fill_table(table, mix_ref)
    nz = home_ref.shape[0]
    home_ref[:, 0] = jnp.zeros_like(kept[0])
    for index, part in enumerate(kept):
        home_ref[:, index + 1] = part[...]
    advance(
        (ping, pong), 0, WIDE + 2 * STEPS, STEPS, rates_ref.at[4], coefficients, table
    )
    take_part(home_ref.at[:, 5], ping, STEPS, size_ref[1])


def table_kernel(cells_ref, weights_ref, out_ref):
    _, columns, wide = out_ref.shape
    capacity = wide // 2
    column = lax.broadcasted_iota(jnp.int32, (columns, capacity), 0)
    for owner in range(out_ref.shape[0]):
        at = slice(owner * capacity, (owner + 1) * capacity)
        table = None
        for corner in range(cells_ref.shape[0]):
            cell = cells_ref[corner : corner + 1, at]
            weight = weights_ref[corner : corner + 1, at]
            term = jnp.where(column == cell, weight, 0.0)
            table = term if table is None else table + term
        high, low = halves(table)
        out_ref[owner, :, :capacity] = high
        out_ref[owner, :, capacity:] = low


def observe_kernel(
    planes, odd_ref, strips_ref, forcing_ref, table_ref, state_ref, out_ref,
    turned, split, tables, arrived,
):
    levels, width_x, width_y = forcing_ref.shape
    owners, _, capacity = out_ref.shape

    def fetch(owner):
        return pltpu.make_async_copy(table_ref.at[owner], tables.at[owner], arrived.at[owner])

    for owner in range(owners):
        fetch(owner).start()
    odd = odd_ref[0]
    starts = starts_of(width_y, planes)
    for j in range(planes):
        place = jnp.where(odd == 1, planes - 1 - j, j)
        turned[starts[j] : starts[j] + WIDE] = strips_ref[place]
    for x in range(width_x):
        value = turned[:, x, :].T + forcing_ref[:, x, :]
        state_ref[:, x, :] = value
        high, low = halves(value)
        split[0:levels, x * width_y : (x + 1) * width_y] = high
        split[levels:, x * width_y : (x + 1) * width_y] = low

    def observe(owner, carry):
        fetch(owner).wait()
        both = jnp.dot(split[...], tables[owner], preferred_element_type=jnp.float32)
        out_ref[owner] = both[:levels, :capacity] + (
            both[:levels, capacity:] + both[levels:, :capacity]
        )
        return carry

    lax.fori_loop(0, owners, observe, 0)


def channel_kernel(table_ref, profile_ref, out_ref):
    table_high, table_low = halves(table_ref[...])
    left = jnp.concatenate([table_high, table_low, table_high], axis=1)
    blocks, _, capacity = profile_ref.shape
    group = 4
    for block in range(0, blocks, group):
        value = jnp.concatenate([profile_ref[block + i] for i in range(group)], axis=1)
        high, low = halves(value)
        right = jnp.concatenate([high, high, low], axis=0)
        out_ref[:, block * capacity : (block + group) * capacity] = jnp.dot(
            left, right, preferred_element_type=jnp.float32
        )


def f32(*shape):
    return jax.ShapeDtypeStruct(shape, jnp.float32)


def local(forcing, winds, mixing, observation_columns, obs_weights, obs_counts, jacobian):
    slots = lax.axis_size("slot")
    halves_z = lax.axis_size("zhi")
    parts_x = lax.axis_size("x")
    owners = lax.axis_size("obs")
    planes = slots * halves_z
    rounds = slots - 1
    block = forcing[0]
    levels, width_x, width_y = block.shape
    whole_x = width_x * parts_x * halves_z
    starts = starts_of(width_y, planes)

    place_o = lax.axis_index("obs")
    place_z = lax.axis_index("zhi") * slots + lax.axis_index("slot")
    odd = (place_o % 2).astype(jnp.int32)
    strip = jnp.where(odd == 1, planes - 1 - place_z, place_z)
    size = (width_y * (strip + 1)) // planes - (width_y * strip) // planes
    odd = odd.reshape(1)
    below = jnp.where(strip == 0, planes - 1, strip - 1)
    size_low = (width_y * (below + 1)) // planes - (width_y * below) // planes
    sizes = jnp.stack([x.astype(jnp.int32) for x in (size, lax.axis_index("x"), size_low)])

    order = []
    for o in range(owners):
        along = range(planes) if o % 2 == 0 else range(planes - 1, -1, -1)
        order += [((z % slots) * halves_z + z // slots) * owners + o for z in along]
    upward = [(order[i - 1], order[i]) for i in range(len(order))]
    downward = [(target, source) for source, target in upward]
    chain = ("slot", "zhi", "obs")

    rates = winds[:, 0]
    block_far, rates_far = (
        pltpu.with_memory_space_constraint(x, pltpu.HBM) for x in (block, rates)
    )
    cut = pl.pallas_call(
        functools.partial(cut_kernel, planes),
        out_shape=f32(planes, WIDE + 1, width_x, levels),
        in_specs=[SMEM(), VMEM(), VMEM()],
        out_specs=VMEM(),
        scratch_shapes=[pltpu.VMEM((width_y, width_x, levels), jnp.float32)],
        compiler_params=params(8),
        cost_estimate=cost(4000000, 1100000),
        name="cut",
    )(odd, block_far, rates_far)
    strips = lax.all_to_all(cut, ("zhi", "slot"), 0, 0, tiled=True)
    strips = strips.reshape(halves_z, slots, WIDE + 1, width_x, levels)
    first = jnp.concatenate(
        [strips[:, 0, :WIDE], strips[:, 1, :WIDE], strips[:, :rounds, WIDE]], axis=1
    )
    later = strips[:, 2:rounds, :WIDE]
    first = lax.all_to_all(
        jnp.broadcast_to(first, (parts_x,) + first.shape), "x", 0, 0, tiled=True
    ).reshape((parts_x,) + first.shape)
    later = lax.all_to_all(
        jnp.broadcast_to(later, (parts_x,) + later.shape), "x", 0, 0, tiled=True
    ).reshape((parts_x,) + later.shape)

    strip = f32(WIDE, whole_x, levels)
    far = pltpu.HBM((WIDE, whole_x, levels), jnp.float32)
    edge = f32(REACH + STEPS, whole_x, levels)
    first_edge = f32(REACH + STEPS + 1, whole_x, levels)
    last_edge = f32(STEPS, whole_x, levels)
    part = f32(halves_z, WIDE, width_x, levels)
    own, mid, up, down, rates = pl.pallas_call(
        spread_kernel,
        out_shape=(far, far, first_edge, first_edge, f32(whole_x, levels)),
        in_specs=[SMEM(), VMEM()],
        out_specs=(VMEM(),) * 5,
        compiler_params=params(8),
        cost_estimate=cost(1000000, 2500000),
        name="spread",
    )(sizes, first)

    turned_mixing = mixing.T
    table = pltpu.VMEM((3 * levels, levels), jnp.bfloat16)

    def window(rows):
        return pltpu.VMEM((rows, whole_x, levels), jnp.float32)

    long = WIDE + 2 * REACH
    short = WIDE + 2 * STEPS
    long_scratch = [window(long)] * 2 + [window(short), table] + [window(long)] * 4
    short_scratch = [window(short)] * 2 + [table] + [window(short)] * 4

    low = lax.ppermute(up, chain, upward)
    high = lax.ppermute(down, chain, downward)
    own, mid = (pltpu.with_memory_space_constraint(x, pltpu.HBM) for x in (own, mid))
    own, mid, end, up, down, *kept, rates = pl.pallas_call(
        early_kernel,
        out_shape=(strip, strip, strip, edge, edge, part, part, f32(rounds, whole_x, levels)),
        in_specs=[SMEM()] + [VMEM()] * 7,
        out_specs=(VMEM(),) * 8,
        scratch_shapes=long_scratch,
        compiler_params=params(24),
        cost_estimate=cost(900000000, 4000000),
        name="early",
    )(sizes, own, mid, low, high, rates, turned_mixing, later)
    low = lax.ppermute(up, chain, upward)
    high = lax.ppermute(down, chain, downward)
    own, up, down, *kept[2:] = pl.pallas_call(
        middle_kernel,
        out_shape=(strip, last_edge, last_edge, part, part),
        in_specs=[SMEM()] + [VMEM()] * 7,
        out_specs=(VMEM(),) * 5,
        scratch_shapes=long_scratch,
        compiler_params=params(24),
        cost_estimate=cost(900000000, 4000000),
        name="middle",
    )(sizes, own, mid, low, high, rates, turned_mixing, end)
    low = lax.ppermute(up, chain, upward)
    high = lax.ppermute(down, chain, downward)
    home = pl.pallas_call(
        late_kernel,
        out_shape=f32(halves_z, slots, WIDE, width_x, levels),
        in_specs=[SMEM()] + [VMEM()] * 9,
        out_specs=VMEM(),
        scratch_shapes=short_scratch,
        compiler_params=params(24),
        cost_estimate=cost(400000000, 3000000),
        name="late",
    )(sizes, own, low, high, rates, turned_mixing, *kept)

    cells = observation_columns[:, 0]
    points, row_count = cells.shape
    capacity = row_count // owners
    live = lax.broadcasted_iota(jnp.int32, (owners, capacity), 1) < obs_counts[0, 0][:, None]
    weights = jnp.where(live.reshape(1, row_count), obs_weights[:, 0], 0.0)
    home, weights = lax.optimization_barrier((home, weights))
    home = home.reshape(planes, WIDE, width_x, levels)
    home = lax.all_to_all(home, ("zhi", "slot"), 0, 0, tiled=True)

    columns = width_x * width_y
    group = 2
    tables = pl.pallas_call(
        table_kernel,
        out_shape=pltpu.HBM((owners, columns, 2 * capacity), jnp.bfloat16),
        grid=(owners // group,),
        in_specs=[pl.BlockSpec((points, group * capacity), lambda q: (0, q))] * 2,
        out_specs=pl.BlockSpec((group, columns, 2 * capacity), lambda q: (q, 0, 0)),
        compiler_params=params(20),
        cost_estimate=cost(1000000000, 8500000),
        name="table",
    )(cells, weights)
    tables = pltpu.with_memory_space_constraint(tables, pltpu.HBM)
    state, profile = pl.pallas_call(
        functools.partial(observe_kernel, planes),
        out_shape=(f32(levels, width_x, width_y), f32(owners, levels, capacity)),
        in_specs=[SMEM(), VMEM(), VMEM(), pl.BlockSpec(memory_space=pltpu.HBM)],
        out_specs=(VMEM(), VMEM()),
        scratch_shapes=[
            pltpu.VMEM((width_y, width_x, levels), jnp.float32),
            pltpu.VMEM((2 * levels, columns), jnp.bfloat16),
            pltpu.VMEM((owners, columns, 2 * capacity), jnp.bfloat16),
            pltpu.SemaphoreType.DMA((owners,)),
        ],
        compiler_params=params(20),
        cost_estimate=cost(2000000000, 11000000),
        name="observe",
    )(odd, home, block, tables)

    profile = lax.all_to_all(profile, "obs", 0, 0, tiled=True)
    channels = jacobian.shape[2]
    radiance = pl.pallas_call(
        channel_kernel,
        out_shape=f32(channels, row_count),
        in_specs=[VMEM()] * 2,
        out_specs=VMEM(),
        compiler_params=params(12),
        cost_estimate=cost(200000000, 2200000),
        name="channel",
    )(jacobian[0, 0], profile)
    return (state[None], radiance[None])


def solution(mesh):
    slots, tiles, owners = (mesh.shape[name] for name in ("slot", "tile", "obs"))
    fine = Mesh(
        mesh.devices.reshape(slots, 2, tiles // 2, owners), ("slot", "zhi", "x", "obs")
    )
    tile = ("zhi", "x")
    return jax.shard_map(
        local,
        mesh=fine,
        in_specs=(
            P("slot", None, tile, "obs"),
            P(None, "slot", tile, "obs"),
            P(),
            P(None, "slot", tile + ("obs",)),
            P(None, "slot", tile + ("obs",)),
            P("slot", tile + ("obs",), None),
            P("slot", "obs", None, None),
        ),
        out_specs=(P("slot", None, tile, "obs"), P("slot", None, tile + ("obs",))),
        check_vma=False,
    )
```

```python
import functools

import jax
import jax.numpy as jnp
from jax import lax
from jax.experimental import pallas as pl
from jax.experimental.pallas import tpu as pltpu
from jax.sharding import Mesh
from jax.sharding import PartitionSpec as P

STEPS = 4
REACH = 2 * STEPS
WIDE = 11
LANE_B = 32

mixing_rate = 0.15

SMEM = functools.partial(pl.BlockSpec, memory_space=pltpu.SMEM)
VMEM = functools.partial(pl.BlockSpec, memory_space=pltpu.VMEM)


def params(mebibytes):
    return pltpu.CompilerParams(vmem_limit_bytes=mebibytes << 20)


def cost(flops, moved):
    return pl.CostEstimate(flops=flops, bytes_accessed=moved, transcendentals=0)


def starts_of(width, planes):
    return [width * j // planes for j in range(planes + 1)]


def halves(x):
    high = x.astype(jnp.bfloat16)
    low = (x - high.astype(jnp.float32)).astype(jnp.bfloat16)
    return high, low


def cut_kernel(planes, odd_ref, forcing_ref, rates_ref, out_ref, turned):
    levels, width_x, width_y = forcing_ref.shape
    odd = odd_ref[0]
    for x in range(width_x):
        turned[:, x, :] = forcing_ref[:, x, :].T
    lane = lax.broadcasted_iota(jnp.int32, (width_x, width_y), 1)
    for j, start in enumerate(starts_of(width_y, planes)[:-1]):
        place = jnp.where(odd == 1, planes - 1 - j, j)
        out_ref[place, 0:WIDE] = turned[start : start + WIDE]
        east = pltpu.roll(rates_ref[0], (width_y - start) % width_y, 1)
        north = pltpu.roll(rates_ref[1], (width_y + WIDE - start) % width_y, 1)
        both = jnp.where(lane < WIDE, east, north)
        out_ref[place, WIDE] = jnp.where(lane < 2 * WIDE, both, 0.0)


def edges(size, up_ref, down_ref, state_ref, forcing_ref=None):
    depth = REACH if forcing_ref is not None else STEPS
    down_ref[0:depth] = state_ref[0:depth]
    up_ref[0:depth] = state_ref[pl.ds(size - depth, depth)]
    if forcing_ref is not None:
        down_ref[depth : depth + STEPS] = forcing_ref[0:STEPS]
        up_ref[depth : depth + STEPS] = forcing_ref[pl.ds(size - STEPS, STEPS)]


def spread_kernel(size_ref, first_ref, own_ref, next_ref, up_ref, down_ref, rates_ref):
    nx, nz, rows, part, _ = first_ref.shape
    for z in range(nz):
        for x in range(nx):
            at = (z * nx + x) * part
            own_ref[:, at : at + part, :] = first_ref[x, z, 0:WIDE]
            next_ref[:, at : at + part, :] = first_ref[x, z, WIDE : 2 * WIDE]
            packed = first_ref[x, z, 2 * WIDE]
            for s in range(1, rows - 2 * WIDE):
                packed = packed + pltpu.roll(first_ref[x, z, 2 * WIDE + s], 2 * WIDE * s, 1)
            rates_ref[at : at + part, :] = packed
    edges(size_ref[0], up_ref, down_ref, own_ref, next_ref)
    down_ref[REACH + STEPS] = rates_ref[...]
    up_ref[REACH + STEPS] = rates_ref[...]


def widen_rates(out_ref, size_ref, own, low, high):
    shape = own.shape
    lanes = shape[1]
    size, size_low = size_ref[0], size_ref[2]
    lane = lax.broadcasted_iota(jnp.int32, shape, 1)
    first = lane < LANE_B
    place = jnp.where(first, lane, lane - LANE_B)

    def moved(value, base, shift):
        east = pltpu.roll(value, lax.rem(shift - base + 2 * lanes, lanes), 1)
        north = pltpu.roll(value, lax.rem(shift + LANE_B - WIDE - base + 2 * lanes, lanes), 1)
        return jnp.where(first, east, north)

    for s in range(out_ref.shape[0]):
        base = jnp.int32(2 * WIDE * s)
        below = moved(low, base, REACH - size_low)
        within = moved(own, base, jnp.int32(REACH))
        above = moved(high, base, REACH + size)
        out_ref[s] = jnp.where(
            place < REACH, below, jnp.where(place < REACH + size, within, above)
        )


def fill_window(window, reach, size, own, low, high):
    window[0:reach] = low
    window[reach : reach + WIDE] = own
    window[reach + WIDE + reach - 1] = jnp.zeros(window.shape[1:], jnp.float32)
    window[pl.ds(reach + size, reach)] = high


def fill_table(table, mix_ref):
    levels = mix_ref.shape[0]
    mix_high, mix_low = halves(mix_ref[...])
    table[0:levels] = mix_high
    table[levels : 2 * levels] = mix_high
    table[2 * levels :] = mix_low


def advance(bufs, first, end, lane, rate, rate_refs, table):
    _, whole_x, levels = bufs[0].shape
    to_east, to_west, to_north, to_south = rate_refs
    shape = (whole_x, levels)
    for y in range(first + 1, end - 1):
        east = jnp.broadcast_to(rate[:, lane + y : lane + y + 1], shape)
        north = jnp.broadcast_to(rate[:, LANE_B + lane + y : LANE_B + lane + y + 1], shape)
        to_east[y] = mixing_rate + east
        to_west[y] = mixing_rate - east
        to_north[y] = mixing_rate + north
        to_south[y] = mixing_rate - north
    for step in range(STEPS):
        source, target = bufs[step % 2], bufs[(step + 1) % 2]
        low, high = first + step + 1, end - step - 1
        for y in range(low, high):
            centre = source[y]
            eastern = pltpu.roll(centre, whole_x - 1, 0)
            western = pltpu.roll(centre, 1, 0)
            across = to_east[y] * eastern + to_west[y] * western
            along = to_north[y] * source[y + 1] + to_south[y] * source[y - 1]
            target[y] = (1.0 - 4.0 * mixing_rate) * centre + (across + along)
        count = high - low
        z = target[low:high].reshape(count * whole_x, levels)
        z_high, z_low = halves(z)
        z = z + jnp.dot(
            jnp.concatenate([z_high, z_low, z_high], axis=1),
            table[...],
            preferred_element_type=jnp.float32,
        )
        target[low:high] = z.reshape(count, whole_x, levels)


def take_part(part_ref, window, reach, x_place):
    nz, _, part, _ = part_ref.shape
    whole_x = window.shape[1]
    for z in range(nz):
        at = pl.multiple_of(z * (whole_x // nz) + x_place * part, part)
        part_ref[z] = window[reach : reach + WIDE, pl.ds(at, part), :]


def gather_x(out_ref, later_ref, index):
    nx, nz, _, _, part, _ = later_ref.shape
    for z in range(nz):
        for x in range(nx):
            at = (z * nx + x) * part
            out_ref[:, at : at + part, :] = later_ref[x, z, index]


def two_slots(size_ref, own_ref, mid_ref, low_ref, high_ref, rates, mix_ref, parts, scratch):
    ping, pong, force, table = scratch[:4]
    coefficients = scratch[4:]
    size, x_place = size_ref[0], size_ref[1]
    fill_window(ping, REACH, size, own_ref[...], low_ref[0:REACH], high_ref[0:REACH])
    fill_window(
        force, STEPS, size, mid_ref[...], low_ref[REACH : REACH + STEPS],
        high_ref[REACH : REACH + STEPS],
    )
    fill_table(table, mix_ref)
    rows = WIDE + 2 * REACH
    advance((ping, pong), 0, rows, 0, rates[0], coefficients, table)
    take_part(parts[0], ping, REACH, x_place)
    ping[STEPS : rows - STEPS] = ping[STEPS : rows - STEPS] + force[...]
    advance((ping, pong), STEPS, rows - STEPS, 0, rates[1], coefficients, table)
    take_part(parts[1], ping, REACH, x_place)
    return ping[REACH : REACH + WIDE]


def early_kernel(
    size_ref, own_ref, mid_ref, low_ref, high_ref, packed_ref, mix_ref, later_ref,
    next_ref, mid_next_ref, end_next_ref, up_ref, down_ref, part_a, part_b, rates_ref, *scratch,
):
    at = REACH + STEPS
    widen_rates(rates_ref, size_ref, packed_ref[...], low_ref[at], high_ref[at])
    gather_x(next_ref, later_ref, 0)
    gather_x(mid_next_ref, later_ref, 1)
    gather_x(end_next_ref, later_ref, 2)
    moved = two_slots(
        size_ref, own_ref, mid_ref, low_ref, high_ref, (rates_ref.at[0], rates_ref.at[1]),
        mix_ref, (part_a, part_b), scratch,
    )
    next_ref[...] = next_ref[...] + moved
    edges(size_ref[0], up_ref, down_ref, next_ref, mid_next_ref)


def middle_kernel(
    size_ref, own_ref, mid_ref, low_ref, high_ref, rates_ref, mix_ref, end_ref,
    next_ref, up_ref, down_ref, part_a, part_b, *scratch,
):
    moved = two_slots(
        size_ref, own_ref, mid_ref, low_ref, high_ref, (rates_ref.at[2], rates_ref.at[3]),
        mix_ref, (part_a, part_b), scratch,
    )
    next_ref[...] = end_ref[...] + moved
    edges(size_ref[0], up_ref, down_ref, next_ref)


def late_kernel(
    size_ref, own_ref, low_ref, high_ref, rates_ref, mix_ref, *rest
):
    kept, home_ref, (ping, pong, table) = rest[:4], rest[4], rest[5:8]
    coefficients = rest[8:]
    fill_window(ping, STEPS, size_ref[0], own_ref[...], low_ref[...], high_ref[...])
    fill_table(table, mix_ref)
    nz = home_ref.shape[0]
    home_ref[:, 0] = jnp.zeros_like(kept[0])
    for index, part in enumerate(kept):
        home_ref[:, index + 1] = part[...]
    advance(
        (ping, pong), 0, WIDE + 2 * STEPS, STEPS, rates_ref.at[4], coefficients, table
    )
    take_part(home_ref.at[:, 5], ping, STEPS, size_ref[1])


def table_kernel(cells_ref, weights_ref, out_ref):
    _, columns, wide = out_ref.shape
    capacity = wide // 2
    column = lax.broadcasted_iota(jnp.int32, (columns, capacity), 0)
    for owner in range(out_ref.shape[0]):
        at = slice(owner * capacity, (owner + 1) * capacity)
        table = None
        for corner in range(cells_ref.shape[0]):
            cell = cells_ref[corner : corner + 1, at]
            weight = weights_ref[corner : corner + 1, at]
            term = jnp.where(column == cell, weight, 0.0)
            table = term if table is None else table + term
        high, low = halves(table)
        out_ref[owner, :, :capacity] = high
        out_ref[owner, :, capacity:] = low


def observe_kernel(
    planes, odd_ref, strips_ref, forcing_ref, table_ref, state_ref, out_ref,
    turned, split, tables, state, arrived, sent,
):
    levels, width_x, width_y = forcing_ref.shape
    owners, _, capacity = out_ref.shape

    def fetch(owner):
        return pltpu.make_async_copy(table_ref.at[owner], tables.at[owner], arrived.at[owner])

    for owner in range(owners):
        fetch(owner).start()
    odd = odd_ref[0]
    starts = starts_of(width_y, planes)
    for j in range(planes):
        place = jnp.where(odd == 1, planes - 1 - j, j)
        turned[starts[j] : starts[j] + WIDE] = strips_ref[place]
    for x in range(width_x):
        value = turned[:, x, :].T + forcing_ref[:, x, :]
        state[:, x, :] = value
        high, low = halves(value)
        split[0:levels, x * width_y : (x + 1) * width_y] = high
        split[levels:, x * width_y : (x + 1) * width_y] = low
    group = 4

    def observe(trip, carry):
        for member in range(group):
            fetch(trip * group + member).wait()
        for member in range(group):
            owner = trip * group + member
            both = jnp.dot(split[...], tables[owner], preferred_element_type=jnp.float32)
            out_ref[owner] = both[:levels, :capacity] + (
                both[:levels, capacity:] + both[levels:, :capacity]
            )
        return carry

    observe(0, 0)
    leave = pltpu.make_async_copy(state, state_ref, sent)
    leave.start()
    lax.fori_loop(1, owners // group, observe, 0)
    leave.wait()


def channel_kernel(table_ref, profile_ref, out_ref):
    table_high, table_low = halves(table_ref[...])
    left = jnp.concatenate([table_high, table_low, table_high], axis=1)
    blocks, _, capacity = profile_ref.shape
    group = 4
    for block in range(0, blocks, group):
        value = jnp.concatenate([profile_ref[block + i] for i in range(group)], axis=1)
        high, low = halves(value)
        right = jnp.concatenate([high, high, low], axis=0)
        out_ref[:, block * capacity : (block + group) * capacity] = jnp.dot(
            left, right, preferred_element_type=jnp.float32
        )


def f32(*shape):
    return jax.ShapeDtypeStruct(shape, jnp.float32)


def local(forcing, winds, mixing, observation_columns, obs_weights, obs_counts, jacobian):
    slots = lax.axis_size("slot")
    halves_z = lax.axis_size("zhi")
    parts_x = lax.axis_size("x")
    owners = lax.axis_size("obs")
    planes = slots * halves_z
    rounds = slots - 1
    block = forcing[0]
    levels, width_x, width_y = block.shape
    whole_x = width_x * parts_x * halves_z
    starts = starts_of(width_y, planes)

    place_o = lax.axis_index("obs")
    place_z = lax.axis_index("zhi") * slots + lax.axis_index("slot")
    odd = (place_o % 2).astype(jnp.int32)
    strip = jnp.where(odd == 1, planes - 1 - place_z, place_z)
    size = (width_y * (strip + 1)) // planes - (width_y * strip) // planes
    odd = odd.reshape(1)
    below = jnp.where(strip == 0, planes - 1, strip - 1)
    size_low = (width_y * (below + 1)) // planes - (width_y * below) // planes
    sizes = jnp.stack([x.astype(jnp.int32) for x in (size, lax.axis_index("x"), size_low)])

    order = []
    for o in range(owners):
        along = range(planes) if o % 2 == 0 else range(planes - 1, -1, -1)
        order += [((z % slots) * halves_z + z // slots) * owners + o for z in along]
    upward = [(order[i - 1], order[i]) for i in range(len(order))]
    downward = [(target, source) for source, target in upward]
    chain = ("slot", "zhi", "obs")

    rates = winds[:, 0]
    block_far, rates_far = (
        pltpu.with_memory_space_constraint(x, pltpu.HBM) for x in (block, rates)
    )
    cut = pl.pallas_call(
        functools.partial(cut_kernel, planes),
        out_shape=f32(planes, WIDE + 1, width_x, levels),
        in_specs=[SMEM(), VMEM(), VMEM()],
        out_specs=VMEM(),
        scratch_shapes=[pltpu.VMEM((width_y, width_x, levels), jnp.float32)],
        compiler_params=params(8),
        cost_estimate=cost(4000000, 1100000),
        name="cut",
    )(odd, block_far, rates_far)
    strips = lax.all_to_all(cut, ("zhi", "slot"), 0, 0, tiled=True)
    strips = strips.reshape(halves_z, slots, WIDE + 1, width_x, levels)
    first = jnp.concatenate(
        [strips[:, 0, :WIDE], strips[:, 1, :WIDE], strips[:, :rounds, WIDE]], axis=1
    )
    later = strips[:, 2:rounds, :WIDE]
    first = lax.all_to_all(
        jnp.broadcast_to(first, (parts_x,) + first.shape), "x", 0, 0, tiled=True
    ).reshape((parts_x,) + first.shape)
    later = lax.all_to_all(
        jnp.broadcast_to(later, (parts_x,) + later.shape), "x", 0, 0, tiled=True
    ).reshape((parts_x,) + later.shape)

    strip = f32(WIDE, whole_x, levels)
    far = pltpu.HBM((WIDE, whole_x, levels), jnp.float32)
    edge = f32(REACH + STEPS, whole_x, levels)
    first_edge = f32(REACH + STEPS + 1, whole_x, levels)
    last_edge = f32(STEPS, whole_x, levels)
    part = f32(halves_z, WIDE, width_x, levels)
    own, mid, up, down, rates = pl.pallas_call(
        spread_kernel,
        out_shape=(far, far, first_edge, first_edge, f32(whole_x, levels)),
        in_specs=[SMEM(), VMEM()],
        out_specs=(VMEM(),) * 5,
        compiler_params=params(8),
        cost_estimate=cost(1000000, 2500000),
        name="spread",
    )(sizes, first)

    turned_mixing = mixing.T
    table = pltpu.VMEM((3 * levels, levels), jnp.bfloat16)

    def window(rows):
        return pltpu.VMEM((rows, whole_x, levels), jnp.float32)

    long = WIDE + 2 * REACH
    short = WIDE + 2 * STEPS
    long_scratch = [window(long)] * 2 + [window(short), table] + [window(long)] * 4
    short_scratch = [window(short)] * 2 + [table] + [window(short)] * 4

    low = lax.ppermute(up, chain, upward)
    high = lax.ppermute(down, chain, downward)
    own, mid = (pltpu.with_memory_space_constraint(x, pltpu.HBM) for x in (own, mid))
    own, mid, end, up, down, *kept, rates = pl.pallas_call(
        early_kernel,
        out_shape=(strip, strip, strip, edge, edge, part, part, f32(rounds, whole_x, levels)),
        in_specs=[SMEM()] + [VMEM()] * 7,
        out_specs=(VMEM(),) * 8,
        scratch_shapes=long_scratch,
        compiler_params=params(24),
        cost_estimate=cost(900000000, 4000000),
        name="early",
    )(sizes, own, mid, low, high, rates, turned_mixing, later)
    low = lax.ppermute(up, chain, upward)
    high = lax.ppermute(down, chain, downward)
    own, up, down, *kept[2:] = pl.pallas_call(
        middle_kernel,
        out_shape=(strip, last_edge, last_edge, part, part),
        in_specs=[SMEM()] + [VMEM()] * 7,
        out_specs=(VMEM(),) * 5,
        scratch_shapes=long_scratch,
        compiler_params=params(24),
        cost_estimate=cost(900000000, 4000000),
        name="middle",
    )(sizes, own, mid, low, high, rates, turned_mixing, end)
    low = lax.ppermute(up, chain, upward)
    high = lax.ppermute(down, chain, downward)
    home = pl.pallas_call(
        late_kernel,
        out_shape=f32(halves_z, slots, WIDE, width_x, levels),
        in_specs=[SMEM()] + [VMEM()] * 9,
        out_specs=VMEM(),
        scratch_shapes=short_scratch,
        compiler_params=params(24),
        cost_estimate=cost(400000000, 3000000),
        name="late",
    )(sizes, own, low, high, rates, turned_mixing, *kept)

    cells = observation_columns[:, 0]
    points, row_count = cells.shape
    capacity = row_count // owners
    live = lax.broadcasted_iota(jnp.int32, (owners, capacity), 1) < obs_counts[0, 0][:, None]
    weights = jnp.where(live.reshape(1, row_count), obs_weights[:, 0], 0.0)
    home, weights = lax.optimization_barrier((home, weights))
    home = home.reshape(planes, WIDE, width_x, levels)
    home = lax.all_to_all(home, ("zhi", "slot"), 0, 0, tiled=True)

    columns = width_x * width_y
    group = 2
    tables = pl.pallas_call(
        table_kernel,
        out_shape=pltpu.HBM((owners, columns, 2 * capacity), jnp.bfloat16),
        grid=(owners // group,),
        in_specs=[pl.BlockSpec((points, group * capacity), lambda q: (0, q))] * 2,
        out_specs=pl.BlockSpec((group, columns, 2 * capacity), lambda q: (q, 0, 0)),
        compiler_params=params(20),
        cost_estimate=cost(1000000000, 8500000),
        name="table",
    )(cells, weights)
    tables = pltpu.with_memory_space_constraint(tables, pltpu.HBM)
    state, profile = pl.pallas_call(
        functools.partial(observe_kernel, planes),
        out_shape=(f32(levels, width_x, width_y), f32(owners, levels, capacity)),
        in_specs=[SMEM(), VMEM(), VMEM(), pl.BlockSpec(memory_space=pltpu.HBM)],
        out_specs=(pl.BlockSpec(memory_space=pltpu.HBM), VMEM()),
        scratch_shapes=[
            pltpu.VMEM((width_y, width_x, levels), jnp.float32),
            pltpu.VMEM((2 * levels, columns), jnp.bfloat16),
            pltpu.VMEM((owners, columns, 2 * capacity), jnp.bfloat16),
            pltpu.VMEM((levels, width_x, width_y), jnp.float32),
            pltpu.SemaphoreType.DMA((owners,)),
            pltpu.SemaphoreType.DMA,
        ],
        compiler_params=params(20),
        cost_estimate=cost(2000000000, 11000000),
        name="observe",
    )(odd, home, block, tables)

    profile = lax.all_to_all(profile, "obs", 0, 0, tiled=True)
    channels = jacobian.shape[2]
    radiance = pl.pallas_call(
        channel_kernel,
        out_shape=f32(channels, row_count),
        in_specs=[VMEM()] * 2,
        out_specs=VMEM(),
        compiler_params=params(12),
        cost_estimate=cost(200000000, 2200000),
        name="channel",
    )(jacobian[0, 0], profile)
    return (state[None], radiance[None])


def solution(mesh):
    slots, tiles, owners = (mesh.shape[name] for name in ("slot", "tile", "obs"))
    fine = Mesh(
        mesh.devices.reshape(slots, 2, tiles // 2, owners), ("slot", "zhi", "x", "obs")
    )
    tile = ("zhi", "x")
    return jax.shard_map(
        local,
        mesh=fine,
        in_specs=(
            P("slot", None, tile, "obs"),
            P(None, "slot", tile, "obs"),
            P(),
            P(None, "slot", tile + ("obs",)),
            P(None, "slot", tile + ("obs",)),
            P("slot", tile + ("obs",), None),
            P("slot", "obs", None, None),
        ),
        out_specs=(P("slot", None, tile, "obs"), P("slot", None, tile + ("obs",))),
        check_vma=False,
    )
```
